32 devices in a mesh: row: 4 (over y, x), col: 8 (over z, core).
Axes of the slice: x: 2, y: 2, z: 4, core: 2. Of those that a mesh axis runs over, the one named last changes fastest.
Arguments:
- model_gradient: float32 [3, 512, 512, 256], P(None, 'row', 'col'), may hold values from -6 to 6
- filter_x: float32 [512, 512], replicated, may hold values from 0 to 1, as said below
- filter_y: float32 [512, 512], replicated, may hold values from 0 to 1, as said below
- filter_z: float32 [256, 256], replicated, may hold values from 0 to 1, as said below
- depth_scale: float32 [3, 256], replicated, may hold values from 0.3 to 3
Outputs:
- smoothed: float32 [3, 512, 512, 256], P(None, 'row', 'col')
The draws below stay inside these ranges and needn't reach their ends.
Inputs may be any that keep to these rules, and one draw needn't show every extreme that they name: `filter_x`: each row is a nonnegative smoothing kernel of its own width plus one half on the diagonal; rows sum to one. `filter_y`: each row is a nonnegative smoothing kernel of its own width plus one half on the diagonal; rows sum to one. `filter_z`: each row is a nonnegative smoothing kernel of its own width plus one half on the diagonal; rows sum to one.
All inputs are finite; a program needn't handle non-finite values.
Results may differ from the reference program's by a relative error of at most 0.0001.
Values sent between devices are 32-bit elements; how exact they have to be, the bound alone decides.
A program may use at most 192 MiB of HBM per device.

```python
import math
import jax
import jax.numpy as jnp
from jax import lax

PARAMS = 3
NX = 512
NY = 512
NZ = 256


def smoothing_matrix(key, length):
    key_width = jax.random.fold_in(key, 11)
    key_rough = jax.random.fold_in(key, 12)
    lower, upper = (0.5, 1.5)
    widths = length * jnp.exp(jax.random.uniform(key_width, (length, 1), jnp.float32, jnp.log(1.0 / 16.0), jnp.log(1.0 / 4.0)))
    places = jnp.arange(length, dtype=jnp.float32)
    apart = places[:, None] - places[None, :]
    rough = jax.random.uniform(key_rough, (length, length), jnp.float32, lower, upper)
    kernel = jnp.exp(-apart * apart / (2.0 * widths * widths)) * rough
    kernel = 0.5 * kernel / jnp.sum(kernel, axis=1, keepdims=True)
    return kernel + 0.5 * jnp.eye(length, dtype=jnp.float32)


def draw_filter_x(key, part):
    return smoothing_matrix(jax.random.fold_in(key, 1), NX)


def draw_filter_y(key, part):
    return smoothing_matrix(jax.random.fold_in(key, 2), NY)


def draw_filter_z(key, part):
    return smoothing_matrix(jax.random.fold_in(key, 3), NZ)


def steps_of(rng, dims, pieces, smallest, high):
    factor_of = 1.0
    for position, blocks in pieces:
        heights = jax.random.uniform(jax.random.fold_in(jax.random.fold_in(rng, 6), position), (blocks,), jnp.float32, smallest / len(pieces), high / len(pieces))
        factor_of = factor_of * jnp.repeat(jnp.exp(heights), dims[position] // blocks).reshape((-1,) + (1,) * (len(dims) - 1 - position))
    return factor_of


def normal_values(key, dims, deviation, limit, cuts=(), held_as=jnp.bfloat16):
    gain = steps_of(key, dims, cuts, -0.22, 0.18) if cuts else 1.0
    result = jax.random.normal(key, dims, jnp.float32) * deviation * gain
    return jnp.minimum(jnp.maximum(result, -limit), limit).astype(held_as)


def setup_inputs(seed: int = 0) -> dict:
    keys = jax.random.split(jax.random.key(seed), 6)
    return {
        "model_gradient": normal_values(keys[0], (PARAMS, NX, NY, NZ), 1.0, 6.0, ((1, 4), (2, 8)), jnp.float32),
        "filter_x": draw_filter_x(jax.random.fold_in(keys[5], 71), 0),
        "filter_y": draw_filter_y(jax.random.fold_in(keys[5], 71), 0),
        "filter_z": draw_filter_z(jax.random.fold_in(keys[5], 71), 0),
        "depth_scale": jnp.clip(jnp.exp(jax.random.uniform(keys[4], (PARAMS, NZ), jnp.float32, math.log(0.3), math.log(3.0))), 0.3, 3.0),
    }


def reference(model_gradient, filter_x, filter_y, filter_z, depth_scale):
    highest_accuracy = lax.Precision.HIGHEST
    results = []
    for index in range(PARAMS):
        field = model_gradient[index]
        depth_pass = jnp.einsum("abz,kz->abk", field, filter_z, precision=highest_accuracy)
        depth_pass = depth_pass * depth_scale[index][None, None, :]
        initial_sweep = jnp.einsum("ia,abk->ibk", filter_x, depth_pass, precision=highest_accuracy)
        second_pass = jnp.einsum("jb,ibk->ijk", filter_y, initial_sweep, precision=highest_accuracy)
        results.append(second_pass)
    return jnp.stack(results)
```

```python
import jax
import jax.numpy as jnp
from jax import lax
from jax.experimental import pallas as pl
from jax.experimental.pallas import tpu as pltpu
from jax.sharding import PartitionSpec as P

ACCURACY = lax.Precision.HIGH
AXES = ("row", "col")
LAST = (((1,), (1,)), ((), ()))
INNER = (((1,), (0,)), ((), ()))


def split_outside(value):
    high = lax.reduce_precision(value, 8, 7)
    return high.astype(jnp.bfloat16), (value - high).astype(jnp.bfloat16)


def split(value):
    high = value.astype(jnp.bfloat16)
    return high, (value - high.astype(jnp.float32)).astype(jnp.bfloat16)


def dot3(left, right, dims):
    def one(a, b):
        return lax.dot_general(a, b, dims, preferred_element_type=jnp.float32)

    return one(left[0], right[0]) + (one(left[0], right[1]) + one(left[1], right[0]))


def cost(flops, count):
    return pl.CostEstimate(flops=flops, bytes_accessed=count, transcendentals=0)


def depth_kernel(high_ref, low_ref, field_ref, out_ref):
    _, xloc, tile, depth = field_ref.shape
    parts, _, block, _ = out_ref.shape
    filters = (high_ref[0], low_ref[0])
    for b in range(tile):
        piece = split(field_ref[0, :, b, :])
        column = dot3(filters, piece, LAST)
        out_ref[:, b] = column.reshape(parts, block, xloc)


def depth_pass(index, high, low, field, parts, tile):
    _, xloc, yloc, depth = field.shape
    block = depth // parts
    return pl.pallas_call(
        depth_kernel,
        grid=(yloc // tile,),
        in_specs=[
            pl.BlockSpec((1, depth, depth), lambda j: (index, 0, 0)),
            pl.BlockSpec((1, depth, depth), lambda j: (index, 0, 0)),
            pl.BlockSpec((1, xloc, tile, depth), lambda j: (index, 0, j, 0)),
        ],
        out_specs=pl.BlockSpec((parts, tile, block, xloc), lambda j: (0, j, 0, 0)),
        out_shape=jax.ShapeDtypeStruct((parts, yloc, block, xloc), jnp.float32),
        cost_estimate=cost(6 * xloc * yloc * depth * depth, 8 * xloc * yloc * depth),
    )(high, low, field)


def first_kernel(high_ref, low_ref, in_ref, out_ref):
    rows, _, yloc, block, xloc = in_ref.shape
    flat = [in_ref[r, 0].reshape(yloc * block, xloc) for r in range(rows)]
    piece = split(jnp.concatenate(flat, axis=1))
    for r in range(rows):
        part = pl.ds(r * xloc, xloc)
        value = dot3(piece, (high_ref[part, :], low_ref[part, :]), LAST)
        out_ref[r, 0] = value.reshape(yloc, block, xloc)


def first_pass(high, low, field):
    rows, cols, yloc, block, xloc = field.shape
    size = rows * xloc
    spec = pl.BlockSpec((rows, 1, yloc, block, xloc), lambda s: (0, s, 0, 0, 0))
    whole = pl.BlockSpec((size, size), lambda s: (0, 0))
    return pl.pallas_call(
        first_kernel,
        grid=(cols,),
        in_specs=[whole, whole, spec],
        out_specs=spec,
        out_shape=jax.ShapeDtypeStruct(field.shape, jnp.float32),
        cost_estimate=cost(6 * size * field.size, 8 * field.size),
    )(high, low, field)


def second_kernel(high_ref, low_ref, in_ref, out_ref):
    _, cols, yloc, block, xloc = in_ref.shape
    size = cols * yloc
    filters = (high_ref[...], low_ref[...])
    for k in range(0, block, 2):
        pair = [in_ref[0, :, :, k + n, :].reshape(size, xloc) for n in range(2)]
        value = dot3(filters, split(jnp.concatenate(pair, axis=1)), INNER)
        for n in range(2):
            part = value[:, n * xloc : (n + 1) * xloc]
            out_ref[0, :, :, k + n, :] = part.reshape(cols, yloc, xloc)


def second_pass(high, low, field):
    rows, cols, yloc, block, xloc = field.shape
    size = cols * yloc
    spec = pl.BlockSpec((1, cols, yloc, block, xloc), lambda r: (r, 0, 0, 0, 0))
    whole = pl.BlockSpec((size, size), lambda r: (0, 0))
    return pl.pallas_call(
        second_kernel,
        grid=(rows,),
        in_specs=[whole, whole, spec],
        out_specs=spec,
        out_shape=jax.ShapeDtypeStruct(field.shape, jnp.float32),
        cost_estimate=cost(6 * size * field.size, 8 * field.size),
    )(high, low, field)


def place_kernel(in_ref, *refs):
    out_ref = refs[-1]
    parts, tile, block, xloc = in_ref.shape
    for j in range(tile):
        plane = in_ref[:, j].reshape(parts * block, xloc)
        out_ref[0, :, j, :] = plane.T


def place(index, params, field, output, tile):
    parts, yloc, block, xloc = field.shape
    depth = parts * block
    given = [] if output is None else [output]
    return pl.pallas_call(
        place_kernel,
        grid=(yloc // tile,),
        in_specs=[pl.BlockSpec((parts, tile, block, xloc), lambda j: (0, j, 0, 0))]
        + [pl.BlockSpec(memory_space=pl.ANY) for _ in given],
        out_specs=pl.BlockSpec((1, xloc, tile, depth), lambda j: (index, 0, j, 0)),
        out_shape=jax.ShapeDtypeStruct((params, xloc, yloc, depth), jnp.float32),
        input_output_aliases={1: 0} if given else {},
        cost_estimate=cost(0, 8 * field.size),
    )(field, *given)


def kernel_shards(model_gradient, filter_x, filter_y, filter_z, depth_scale):
    rows, cols = lax.axis_size("row"), lax.axis_size("col")
    params, xloc, yloc, depth = model_gradient.shape
    parts = rows * cols
    block = depth // parts
    scaled = split_outside(depth_scale[:, :, None] * filter_z[None, :, :])
    pair_x, pair_y = split_outside(filter_x), split_outside(filter_y)
    arrived = []
    for index in range(params):
        outgoing = depth_pass(index, *scaled, model_gradient, parts, 8)
        arrived.append(
            lax.all_to_all(outgoing, AXES, split_axis=0, concat_axis=0, tiled=True)
        )
    output = None
    for index in range(params):
        field = arrived[index].reshape(rows, cols, yloc, block, xloc)
        field = second_pass(*pair_y, first_pass(*pair_x, field))
        field = field.reshape(parts, yloc, block, xloc)
        back = lax.all_to_all(field, AXES, split_axis=0, concat_axis=0, tiled=True)
        output = place(index, params, back, output, 8)
    return output


def plane_filter(incoming, filter_x, filter_y, rows, cols):
    xloc, yloc = incoming.shape[0], incoming.shape[1]
    matrix_x = filter_x.reshape(rows, xloc, rows, xloc)
    matrix_y = filter_y.reshape(cols, yloc, cols, yloc)
    partial_value = jnp.einsum(
        "ABRa,abRSz->ABbSz", matrix_x, incoming, precision=ACCURACY
    )
    return jnp.einsum(
        "CDSb,ABbSz->ACBDz", matrix_y, partial_value, precision=ACCURACY
    )


def plain_shards(model_gradient, filter_x, filter_y, filter_z, depth_scale):
    rows, cols = lax.axis_size("row"), lax.axis_size("col")
    params, xloc, yloc, depth = model_gradient.shape
    parts = rows * cols
    block = depth // parts
    arrived = []
    for index in range(params):
        scaled_filter = depth_scale[index][:, None] * filter_z
        column = jnp.einsum(
            "kz,abz->abk", scaled_filter, model_gradient[index], precision=ACCURACY
        )
        outgoing = column.reshape(xloc, yloc, parts, block)
        arrived.append(
            lax.all_to_all(outgoing, AXES, split_axis=2, concat_axis=2, tiled=True)
        )
    results = []
    for index in range(params):
        incoming = arrived[index].reshape(xloc, yloc, rows, cols, block)
        planes = plane_filter(incoming, filter_x, filter_y, rows, cols)
        planes = planes.reshape(parts, xloc, yloc, block)
        back = lax.all_to_all(planes, AXES, split_axis=0, concat_axis=3, tiled=True)
        results.append(back.reshape(xloc, yloc, depth))
    return jnp.stack(results)


def shards(model_gradient, filter_x, filter_y, filter_z, depth_scale):
    _, xloc, yloc, depth = model_gradient.shape
    block = depth // (lax.axis_size("row") * lax.axis_size("col"))
    aligned = block % 8 == 0 and xloc % 128 == 0 and yloc % 8 == 0
    chosen = kernel_shards if aligned else plain_shards
    return chosen(model_gradient, filter_x, filter_y, filter_z, depth_scale)


def solution(mesh):
    return jax.shard_map(
        shards,
        mesh=mesh,
        in_specs=(P(None, "row", "col", None), P(), P(), P(), P()),
        out_specs=P(None, "row", "col", None),
        check_vma=False,
    )
```
